32 devices in a mesh: chan: 8 (over z, y), slot: 4 (over x, core).
Axes of the slice: x: 2, y: 2, z: 4, core: 2. Of those that a mesh axis runs over, the one named last changes fastest.
Arguments:
- visibility: float32 [2, 2, 32, 4, 3844], P(None, None, 'chan', 'slot'), parts along dimension 3, may hold values from -6 to 6
- coherency: bfloat16 [2, 2, 16, 32, 4, 3844], P(None, None, None, 'chan', 'slot'), parts along dimension 4, may hold values from -2 to 2
- jones_start: float32 [2, 2, 64, 32, 62], P(None, None, 'slot', 'chan'), parts along dimension 2, may hold values from -4 to 4
- duals_start: float32 [2, 2, 64, 32, 62], P(None, None, 'slot', 'chan'), parts along dimension 2, may hold values from -2 to 2
Outputs:
- jones_final: float32 [2, 2, 64, 32, 62], P(None, None, 'slot', 'chan'), parts along dimension 2
- consensus: float32 [2, 2, 64, 32, 62], P(None, None, 'slot', 'chan'), parts along dimension 2
- duals_final: float32 [2, 2, 64, 32, 62], P(None, None, 'slot', 'chan'), parts along dimension 2
- norms: float32 [8, 2], P('slot'), parts along dimension 0
The draws below stay inside these ranges and needn't reach their ends.
There are 4 independent parts, one for each index of `slot`. The reference program is written for one: setup_inputs(seed, part) draws one part's arguments, and reference() takes and returns one part's arrays. A program takes and returns all parts, laid end to end along the dimension named above; each array names one. Nothing has to cross between parts.
All inputs are finite; a program needn't handle non-finite values.
Results may differ from the reference program's by a relative error of at most 0.0003.
Values sent between devices are 32-bit elements; how exact they have to be, the bound alone decides.
A program may use at most 128 MiB of HBM per device.

```python
import jax
import jax.numpy as jnp
from jax import lax

STATIONS = 62
DIRS = 16
POLS = 2
TIMES = 1
ITERS = 2
CH_DEV = 4
CHANNELS = 32
PAIRS = 3844
N_CHAN = 8


def block_levels(key, extent, cuts, low, high):
    def one(dim, shards_of):
        heights = jax.random.uniform(jax.random.fold_in(jax.random.fold_in(key, 6), dim), (shards_of,), jnp.float32, low / len(cuts), high / len(cuts))
        return jnp.repeat(jnp.exp(heights), extent[dim] // shards_of).reshape((-1,) + (1,) * (len(extent) - dim - 1))

    level = one(*cuts[0])
    for cut in cuts[1:]:
        level = level * one(*cut)
    return level


def scatter_about(rng, dims, scale, bound, split=(), kind=jnp.bfloat16):
    values = jax.random.normal(rng, dims, jnp.float32) * scale
    if len(split) > 0:
        values = block_levels(rng, dims, split, -0.22, 0.18) * values
    return jnp.clip(values, min=-bound, max=bound).astype(kind)


def setup_inputs(seed: int = 0, part: int = 0) -> dict:
    key_list = jax.random.split(jax.random.key(seed), 5)
    part_splits = jax.random.split(jax.random.fold_in(key_list[4], part), 5)
    visibility = scatter_about(part_splits[0], (2, POLS, CHANNELS, TIMES, PAIRS), 1.0, 6.0, ((2, 8),), jnp.float32)
    coherency = scatter_about(part_splits[1], (2, POLS, DIRS, CHANNELS, TIMES, PAIRS), 0.25, 2.0, ((3, 8),))
    jones_start = scatter_about(part_splits[2], (2, POLS, DIRS, CHANNELS, STATIONS), 0.7, 4.0, ((3, 8),), jnp.float32)
    duals_start = scatter_about(part_splits[3], (2, POLS, DIRS, CHANNELS, STATIONS), 0.3, 2.0, ((3, 8),), jnp.float32)
    return {"visibility": visibility, "coherency": coherency, "jones_start": jones_start, "duals_start": duals_start}


penalty = 8.0
kernel_taps = (0.04, 0.06, 0.1, 0.15, 0.3, 0.15, 0.1, 0.06, 0.04)


def jones_update(visibility, coherency, jones_now, target):
    width = jones_now.shape[-1]
    grid_shape = coherency.shape[1:5] + (width, width)
    sky_real = coherency[0].astype(jnp.float32).reshape(grid_shape)
    sky_imag = coherency[1].astype(jnp.float32).reshape(grid_shape)
    vis_shape = visibility.shape[1:4] + (width, width)
    data_real = visibility[0].reshape(vis_shape)[:, None]
    data_imag = visibility[1].reshape(vis_shape)[:, None]
    left_real = jones_now[0][:, :, :, None, :, None]
    left_imag = jones_now[1][:, :, :, None, :, None]
    right_real = jones_now[0][:, :, :, None, None, :]
    right_imag = jones_now[1][:, :, :, None, None, :]
    crossed = 1.0 - jnp.eye(width, dtype=jnp.float32)
    half_real = left_real * sky_real - left_imag * sky_imag
    half_imag = left_real * sky_imag + left_imag * sky_real
    model_real = half_real * right_real + half_imag * right_imag
    model_imag = half_imag * right_real - half_real * right_imag
    rest_real = (data_real - jnp.sum(model_real, axis=1, keepdims=True) + model_real) * crossed
    rest_imag = (data_imag - jnp.sum(model_imag, axis=1, keepdims=True) + model_imag) * crossed
    weight_real = sky_real * right_real + sky_imag * right_imag
    weight_imag = sky_real * right_imag - sky_imag * right_real
    upper_real = jnp.sum(rest_real * weight_real - rest_imag * weight_imag, axis=(3, 5))
    upper_imag = jnp.sum(rest_real * weight_imag + rest_imag * weight_real, axis=(3, 5))
    lower = jnp.sum(crossed * (sky_real * sky_real + sky_imag * sky_imag) * (right_real * right_real + right_imag * right_imag), axis=(3, 5)) + penalty
    return jnp.stack([(upper_real + penalty * target[0]) / lower, (upper_imag + penalty * target[1]) / lower])


def blocked_update(visibility, coherency, jones_now, target):
    vis_shape = visibility.shape
    vis_blocks = jnp.moveaxis(visibility.reshape(vis_shape[:2] + (N_CHAN, CH_DEV) + vis_shape[3:]), 2, 0)
    coh_shape = coherency.shape
    coh_blocks = jnp.moveaxis(coherency.reshape(coh_shape[:3] + (N_CHAN, CH_DEV) + coh_shape[4:]), 3, 0)
    gain_shape = jones_now.shape
    gain_blocks = jnp.moveaxis(jones_now.reshape(gain_shape[:3] + (N_CHAN, CH_DEV) + gain_shape[4:]), 3, 0)
    target_blocks = jnp.moveaxis(target.reshape(gain_shape[:3] + (N_CHAN, CH_DEV) + gain_shape[4:]), 3, 0)
    updated = lax.map(lambda blocks_in: jones_update(*blocks_in), (vis_blocks, coh_blocks, gain_blocks, target_blocks))
    return jnp.moveaxis(updated, 0, 3).reshape(gain_shape)


def smooth(padded, channels):
    total = kernel_taps[0] * padded[:, :, :, 0:channels]
    for offset in range(1, 9):
        total = total + kernel_taps[offset] * padded[:, :, :, offset:offset + channels]
    return total


def reference(visibility, coherency, jones_start, duals_start):
    channels = jones_start.shape[3]
    entries = jones_start.size
    jones_now = jones_start
    consensus = jones_start
    duals_now = duals_start
    partials = []
    for iteration in range(ITERS):
        jones_now = blocked_update(visibility, coherency, jones_now, consensus - duals_now)
        summed = jones_now + duals_now
        padded = jnp.pad(summed, ((0, 0), (0, 0), (0, 0), (4, 4), (0, 0)))
        fresh = smooth(padded, channels)
        duals_now = duals_now + jones_now - fresh
        primal_gap = jones_now - fresh
        moved = fresh - consensus
        primal = jnp.sum(primal_gap * primal_gap) / entries
        change = penalty * penalty * jnp.sum(moved * moved) / entries
        partials.append(jnp.stack([primal, change]))
        consensus = fresh
    return jones_now, consensus, duals_now, jnp.stack(partials)
```

```python
import functools

import jax
import jax.numpy as jnp
from jax import lax
from jax.experimental import pallas as pl
from jax.experimental.pallas import tpu as pltpu
from jax.sharding import PartitionSpec as P

ITERS = 2
HALF = 64
BLOCK = 256
MESH = pl.DeviceIdType.MESH

penalty = 8.0
kernel_taps = (0.04, 0.06, 0.1, 0.15, 0.3, 0.15, 0.1, 0.06, 0.04)


def split(value):
    high = value.astype(jnp.bfloat16)
    return high, (value - high.astype(jnp.float32)).astype(jnp.bfloat16)


def spread_tables(width, blocks, spread_p, spread_q, gather_p):
    def fill(b, carry):
        start = pl.multiple_of(b * BLOCK, BLOCK)
        pair = (lax.broadcasted_iota(jnp.int32, (HALF, BLOCK), 1) + start).astype(jnp.float32)
        station = lax.broadcasted_iota(jnp.int32, (HALF, BLOCK), 0).astype(jnp.float32)
        first = jnp.floor((pair + 0.5) * (1.0 / width))
        second = pair - first * width
        keep = (first != second) & (first < width)
        spread_p[:, pl.ds(start, BLOCK)] = jnp.where((first == station) & keep, 1.0, 0.0).astype(jnp.bfloat16)
        spread_q[:, pl.ds(start, BLOCK)] = jnp.where((second == station) & keep, 1.0, 0.0).astype(jnp.bfloat16)
        pair = (lax.broadcasted_iota(jnp.int32, (BLOCK, 2 * HALF), 0) + start).astype(jnp.float32)
        station = (lax.broadcasted_iota(jnp.int32, (BLOCK, 2 * HALF), 1) & (HALF - 1)).astype(jnp.float32)
        inside = pair - station * width
        keep = (inside >= 0.0) & (inside < width) & (inside != station) & (station < width)
        gather_p[pl.ds(start, BLOCK), :] = jnp.where(keep, 1.0, 0.0).astype(jnp.bfloat16)
        return carry

    lax.fori_loop(0, blocks, fill, 0)


def kernel(
    count, dims,
    vis_in, sky_in, jones_in, duals_in,
    jones_out, consensus_out, duals_out, norms_out,
    vis, sky, spread_p, spread_q, gather_p, lhs, left, right, parts,
    gain, cons, dual, total, summed, from_low, from_high, sums, slots,
    send_sem, low_sem, high_sem, norm_send, norm_recv,
):
    pols, dirs, channels, width, pairs, blocks, entries = dims
    me = lax.axis_index("chan")
    rows = pols * channels
    tall = dirs * rows

    for it in range(ITERS):
        from_low[it] = jnp.zeros_like(from_low[it])
        from_high[it] = jnp.zeros_like(from_high[it])
    barrier = pltpu.get_barrier_semaphore()
    for step in range(1, count):
        pl.semaphore_signal(barrier, inc=1, device_id={"chan": lax.rem(me + step, count)}, device_id_type=MESH)

    spread_tables(width, blocks, spread_p, spread_q, gather_p)
    for part in range(2):
        vis[part] = jnp.zeros_like(vis[part])
        for pol in range(pols):
            for chan in range(channels):
                row = pol * channels + chan
                vis[part, row : row + 1, 0:pairs] = vis_in[part, pol, chan]
    tail = pairs // 128 * 128
    edge = blocks * BLOCK - tail
    sky[:, :, :, pl.ds(tail, edge)] = jnp.zeros((2, dirs, rows, edge), jnp.float32)

    def unpack(k, carry):
        for part in range(2):
            for pol in range(pols):
                sky[part, k, pol * channels : (pol + 1) * channels, 0:pairs] = sky_in[part, pol, k].astype(jnp.float32)
        return carry

    lax.fori_loop(0, dirs, unpack, 0)

    gain[...] = jnp.zeros_like(gain)
    dual[...] = jnp.zeros_like(dual)
    for part in range(2):
        for pol in range(pols):
            at = (slice(None), slice(pol * channels, (pol + 1) * channels), slice(part * HALF, part * HALF + width))
            gain[at] = jones_in[part, pol]
            dual[at] = duals_in[part, pol]
    cons[...] = gain[...]
    sums[...] = jnp.zeros_like(sums)

    row = lax.broadcasted_iota(jnp.int32, (rows, 128), 0) % channels

    def taps(distance, shift, low, high):
        offset = distance + shift + 4
        if offset < 0 or offset > 8:
            return None
        inside = (row + shift >= low) & (row + shift < high)
        return jnp.where(inside, kernel_taps[offset], 0.0)

    def mixed(block, distance):
        out = None
        for shift in range(1 - channels, channels):
            weight = taps(distance, shift, 0, channels)
            if weight is None:
                continue
            moved = block if shift == 0 else pltpu.roll(block, (-shift) % rows, 1)
            term = weight[None] * moved
            out = term if out is None else out + term
        return out

    def norm_copy(step):
        return pltpu.make_async_remote_copy(
            src_ref=sums, dst_ref=slots.at[me],
            send_sem=norm_send.at[step], recv_sem=norm_recv.at[step],
            device_id={"chan": lax.rem(me + step, count)}, device_id_type=MESH,
        )

    for it in range(ITERS):
        now = gain[...].reshape(tall, 128)
        high, low = split(now)
        lhs[0:tall, 0:128] = high
        lhs[0:tall, 128:256] = low
        high, low = split(pltpu.roll(now, HALF, 1))
        lhs[tall:, 0:128] = high
        lhs[tall:, 128:256] = low
        total[...] = jnp.zeros_like(total)

        def block_step(b, carry):
            start = pl.multiple_of(b * BLOCK, BLOCK)
            zeros = jnp.zeros((HALF, BLOCK), jnp.bfloat16)
            ep = spread_p[:, pl.ds(start, BLOCK)]
            eq = spread_q[:, pl.ds(start, BLOCK)]
            left[...] = jnp.dot(lhs[...], jnp.concatenate([ep, zeros, ep, zeros], 0), preferred_element_type=jnp.float32)
            right[...] = jnp.dot(lhs[...], jnp.concatenate([eq, zeros, eq, zeros], 0), preferred_element_type=jnp.float32)
            for lane in range(0, BLOCK, 128):
                lanes = pl.ds(pl.multiple_of(start + lane, 128), 128)
                model_r = jnp.zeros((rows, 128), jnp.float32)
                model_i = jnp.zeros((rows, 128), jnp.float32)
                held = []
                for k in range(dirs):
                    sr, si = sky[0, k, :, lanes], sky[1, k, :, lanes]
                    mine = slice(k * rows, (k + 1) * rows)
                    other = slice(tall + k * rows, tall + (k + 1) * rows)
                    here = slice(lane, lane + 128)
                    rr, ri = right[mine, here], right[other, here]
                    lr, li = left[mine, here], left[other, here]
                    zr = sr * rr + si * ri
                    zi = sr * ri - si * rr
                    model_r = model_r + (lr * zr + li * zi)
                    model_i = model_i + (li * zr - lr * zi)
                    held.append((zr, zi))
                dr = vis[0, :, lanes] - model_r
                di = vis[1, :, lanes] - model_i
                for k in range(0, dirs, 2):
                    pair = held[k : k + 2]
                    values = (
                        [dr * zr - di * zi for zr, zi in pair],
                        [dr * zi + di * zr for zr, zi in pair],
                        [zr * zr + zi * zi for zr, zi in pair],
                    )
                    for i, value in enumerate(values):
                        high, low = split(jnp.concatenate(value, 0))
                        at = slice(i * tall + k * rows, i * tall + (k + 2) * rows)
                        parts[0, at, lane : lane + 128] = high
                        parts[1, at, lane : lane + 128] = low
            weight = gather_p[pl.ds(start, BLOCK), :]
            total[...] += jnp.dot(parts[0], weight, preferred_element_type=jnp.float32) + jnp.dot(
                parts[1], weight, preferred_element_type=jnp.float32
            )
            return carry

        lax.fori_loop(0, blocks, block_step, 0)

        lane = lax.broadcasted_iota(jnp.int32, (tall, 128), 1)
        upper = jnp.where(lane < HALF, total[0:tall], total[tall : 2 * tall]).reshape(dirs, rows, 128)
        lower = total[2 * tall :].reshape(dirs, rows, 128)
        fresh_gain = (upper + gain[...] * lower + penalty * (cons[...] - dual[...])) / (lower + penalty)
        gain[...] = fresh_gain
        summed[it] = fresh_gain + dual[...]

        def halo(direction):
            return pltpu.make_async_remote_copy(
                src_ref=summed.at[it],
                dst_ref=(from_low if direction > 0 else from_high).at[it],
                send_sem=send_sem.at[it, 0 if direction > 0 else 1],
                recv_sem=(low_sem if direction > 0 else high_sem).at[it],
                device_id={"chan": lax.rem(me + direction + count, count)}, device_id_type=MESH,
            )

        if it == 0:
            pl.semaphore_wait(barrier, count - 1)
        up, down = halo(1), halo(-1)

        @pl.when(me < count - 1)
        def _():
            up.start()

        @pl.when(me > 0)
        def _():
            down.start()

        own = mixed(summed[it], 0)

        @pl.when(me > 0)
        def _():
            up.wait_recv()

        @pl.when(me < count - 1)
        def _():
            down.wait_recv()

        fresh = own + mixed(from_low[it], -channels) + mixed(from_high[it], channels)
        gap = gain[...] - fresh
        moved = fresh - cons[...]
        dual[...] = dual[...] + gap
        cons[...] = fresh
        primal = jnp.sum(jnp.sum(gap * gap, 0), 0, keepdims=True)
        change = jnp.sum(jnp.sum(moved * moved, 0), 0, keepdims=True)
        sums[2 * it : 2 * it + 1] = primal
        sums[2 * it + 1 : 2 * it + 2] = change

    slots[pl.ds(me, 1)] = sums[...][None]
    for step in range(1, count):
        norm_copy(step).start()

    for part in range(2):
        for pol in range(pols):
            at = (slice(None), slice(pol * channels, (pol + 1) * channels), slice(part * HALF, part * HALF + width))
            jones_out[part, pol] = gain[at]
            consensus_out[part, pol] = cons[at]
            duals_out[part, pol] = dual[at]

    for it in range(ITERS):

        @pl.when(me < count - 1)
        def _():
            pltpu.make_async_remote_copy(
                src_ref=summed.at[it], dst_ref=from_low.at[it], send_sem=send_sem.at[it, 0], recv_sem=low_sem.at[it],
                device_id={"chan": lax.rem(me + 1, count)}, device_id_type=MESH,
            ).wait_send()

        @pl.when(me > 0)
        def _():
            pltpu.make_async_remote_copy(
                src_ref=summed.at[it], dst_ref=from_high.at[it], send_sem=send_sem.at[it, 1], recv_sem=high_sem.at[it],
                device_id={"chan": lax.rem(me - 1 + count, count)}, device_id_type=MESH,
            ).wait_send()

    for step in range(1, count):
        norm_copy(step).wait()
    gathered = slots[0]
    for j in range(1, count):
        gathered = gathered + slots[j]
    folded = jnp.sum(gathered, axis=1, keepdims=True) * (1.0 / entries)
    for it in range(ITERS):
        norms_out[it : it + 1, 0:1] = folded[2 * it : 2 * it + 1]
        norms_out[it : it + 1, 1:2] = folded[2 * it + 1 : 2 * it + 2] * (penalty * penalty)


def solution(mesh):
    count = mesh.shape["chan"]

    def local(visibility, coherency, jones_start, duals_start):
        _, pols, dirs, channels, width = jones_start.shape
        pairs = visibility.shape[-1]
        times = visibility.shape[3]
        assert times == 1 and channels == 4 and pols * channels == 8 and width <= HALF - 2
        blocks = pl.cdiv(pairs, BLOCK)
        long = blocks * BLOCK
        rows, tall = pols * channels, dirs * pols * channels
        entries = jones_start.size * count
        sky = coherency.transpose(0, 1, 2, 4, 3, 5).reshape(2, pols, dirs, channels, pairs)
        state = jax.ShapeDtypeStruct(jones_start.shape, jnp.float32)
        f32, bf16 = jnp.float32, jnp.bfloat16
        packed = (dirs, rows, 2 * HALF)
        return pl.pallas_call(
            functools.partial(kernel, count, (pols, dirs, channels, width, pairs, blocks, entries)),
            out_shape=(state, state, state, jax.ShapeDtypeStruct((ITERS, 2), f32)),
            in_specs=[pl.BlockSpec(memory_space=pltpu.VMEM)] * 4,
            out_specs=tuple([pl.BlockSpec(memory_space=pltpu.VMEM)] * 4),
            scratch_shapes=[
                pltpu.VMEM((2, rows, long), f32),
                pltpu.VMEM((2, dirs, rows, long), f32),
                pltpu.VMEM((HALF, long), bf16),
                pltpu.VMEM((HALF, long), bf16),
                pltpu.VMEM((long, 2 * HALF), bf16),
                pltpu.VMEM((2 * tall, 4 * HALF), bf16),
                pltpu.VMEM((2 * tall, BLOCK), f32),
                pltpu.VMEM((2 * tall, BLOCK), f32),
                pltpu.VMEM((2, 3 * tall, BLOCK), bf16),
                pltpu.VMEM(packed, f32),
                pltpu.VMEM(packed, f32),
                pltpu.VMEM(packed, f32),
                pltpu.VMEM((3 * tall, 2 * HALF), f32),
                pltpu.VMEM((ITERS,) + packed, f32),
                pltpu.VMEM((ITERS,) + packed, f32),
                pltpu.VMEM((ITERS,) + packed, f32),
                pltpu.VMEM((8, 2 * HALF), f32),
                pltpu.VMEM((count, 8, 2 * HALF), f32),
                pltpu.SemaphoreType.DMA((ITERS, 2)),
                pltpu.SemaphoreType.DMA((ITERS,)),
                pltpu.SemaphoreType.DMA((ITERS,)),
                pltpu.SemaphoreType.DMA((count,)),
                pltpu.SemaphoreType.DMA((count,)),
            ],
            compiler_params=pltpu.CompilerParams(
                collective_id=0, has_side_effects=True, vmem_limit_bytes=48 * 1024 * 1024
            ),
        )(visibility, sky, jones_start, duals_start)

    placed = (
        P(None, None, "chan", "slot", None),
        P(None, None, None, "chan", "slot", None),
        P(None, None, "slot", "chan", None),
        P(None, None, "slot", "chan", None),
    )
    return jax.shard_map(
        local,
        mesh=mesh,
        in_specs=placed,
        out_specs=(
            P(None, None, "slot", "chan", None),
            P(None, None, "slot", "chan", None),
            P(None, None, "slot", "chan", None),
            P("slot", None),
        ),
        check_vma=False,
    )
```

```python
import functools

import jax
import jax.numpy as jnp
from jax import lax
from jax.experimental import pallas as pl
from jax.experimental.pallas import tpu as pltpu
from jax.sharding import PartitionSpec as P

ITERS = 2
HALF = 64
BLOCK = 256
UNROLL = 2
MESH = pl.DeviceIdType.MESH

penalty = 8.0
kernel_taps = (0.04, 0.06, 0.1, 0.15, 0.3, 0.15, 0.1, 0.06, 0.04)


def split(value):
    high = value.astype(jnp.bfloat16)
    return high, (value - high.astype(jnp.float32)).astype(jnp.bfloat16)


def spread_tables(width, blocks, spread_p, spread_q, gather_p):
    def fill(b, carry):
        start = pl.multiple_of(b * BLOCK, BLOCK)
        pair = (lax.broadcasted_iota(jnp.int32, (HALF, BLOCK), 1) + start).astype(jnp.float32)
        station = lax.broadcasted_iota(jnp.int32, (HALF, BLOCK), 0).astype(jnp.float32)
        first = jnp.floor((pair + 0.5) * (1.0 / width))
        second = pair - first * width
        keep = (first != second) & (first < width)
        spread_p[:, pl.ds(start, BLOCK)] = jnp.where((first == station) & keep, 1.0, 0.0).astype(jnp.bfloat16)
        spread_q[:, pl.ds(start, BLOCK)] = jnp.where((second == station) & keep, 1.0, 0.0).astype(jnp.bfloat16)
        pair = (lax.broadcasted_iota(jnp.int32, (BLOCK, 2 * HALF), 0) + start).astype(jnp.float32)
        station = (lax.broadcasted_iota(jnp.int32, (BLOCK, 2 * HALF), 1) & (HALF - 1)).astype(jnp.float32)
        inside = pair - station * width
        keep = (inside >= 0.0) & (inside < width) & (inside != station) & (station < width)
        gather_p[pl.ds(start, BLOCK), :] = jnp.where(keep, 1.0, 0.0).astype(jnp.bfloat16)
        return carry

    lax.fori_loop(0, blocks, fill, 0)


def kernel(
    count, dims,
    vis_in, sky_in, jones_in, duals_in,
    jones_out, consensus_out, duals_out, norms_out,
    vis_raw, sky_raw, jones_raw, duals_raw,
    vis, sky, spread_p, spread_q, gather_p, lhs, left, right, parts,
    gain, cons, dual, total, summed, from_low, from_high, sums, slots,
    load_sem, sky_sem, send_sem, low_sem, high_sem, norm_send, norm_recv,
):
    pols, dirs, channels, width, pairs, blocks, entries = dims
    me = lax.axis_index("chan")
    group = 8 // channels
    tiles = dirs // group
    tall = tiles * 8

    loads = [
        pltpu.make_async_copy(source, target, load_sem.at[i])
        for i, (source, target) in enumerate(((vis_in, vis_raw), (jones_in, jones_raw), (duals_in, duals_raw)))
    ]
    sky_loads = [
        [pltpu.make_async_copy(sky_in.at[part, pol], sky_raw.at[part, pol], sky_sem.at[part, pol]) for part in range(2)]
        for pol in range(pols)
    ]
    for copy in loads + [copy for per_pol in sky_loads for copy in per_pol]:
        copy.start()

    from_low[...] = jnp.zeros_like(from_low)
    from_high[...] = jnp.zeros_like(from_high)
    barrier = pltpu.get_barrier_semaphore()
    for step in range(1, count):
        pl.semaphore_signal(barrier, inc=1, device_id={"chan": lax.rem(me + step, count)}, device_id_type=MESH)

    spread_tables(width, blocks, spread_p, spread_q, gather_p)
    tail = pairs // 128 * 128
    edge = blocks * BLOCK - tail
    vis[:, :, :, pl.ds(tail, edge)] = jnp.zeros((2, pols, 8, edge), jnp.float32)
    sky[:, :, :, :, pl.ds(tail, edge)] = jnp.zeros((2, pols, tiles, 8, edge), jnp.float32)
    gain[...] = jnp.zeros_like(gain)
    dual[...] = jnp.zeros_like(dual)
    sums[...] = jnp.zeros_like(sums)
    for copy in loads:
        copy.wait()
    for part in range(2):
        for pol in range(pols):
            for row in range(8):
                vis[part, pol, row : row + 1, 0:pairs] = vis_raw[part, pol, row % channels]
            for lead in range(group):
                rows = slice(lead * channels, (lead + 1) * channels)
                lanes = slice(part * HALF, part * HALF + width)
                for tile in range(tiles):
                    gain[pol, tile, rows, lanes] = jones_raw[part, pol, tile * group + lead]
                    dual[pol, tile, rows, lanes] = duals_raw[part, pol, tile * group + lead]
    cons[...] = gain[...]

    def unpack(pol):
        for copy in sky_loads[pol]:
            copy.wait()

        def one(tile, carry):
            for part in range(2):
                for lead in range(group):
                    rows = slice(lead * channels, (lead + 1) * channels)
                    sky[part, pol, tile, rows, 0:pairs] = sky_raw[part, pol, tile * group + lead].astype(jnp.float32)
            return carry

        lax.fori_loop(0, tiles, one, 0)

    def solve(pol):
        now = gain[pol].reshape(tall, 128)
        high, low = split(now)
        lhs[pol, 0:tall, 0:128] = high
        lhs[pol, 0:tall, 128:256] = low
        high, low = split(pltpu.roll(now, HALF, 1))
        lhs[pol, tall:, 0:128] = high
        lhs[pol, tall:, 128:256] = low
        total[...] = jnp.zeros_like(total)

        def one_block(start, u):
            zeros = jnp.zeros((HALF, BLOCK), jnp.bfloat16)
            ep = spread_p[:, pl.ds(start, BLOCK)]
            eq = spread_q[:, pl.ds(start, BLOCK)]
            gains = lhs[pol]
            left[u] = jnp.dot(gains, jnp.concatenate([ep, zeros, ep, zeros], 0), preferred_element_type=jnp.float32)
            right[u] = jnp.dot(gains, jnp.concatenate([eq, zeros, eq, zeros], 0), preferred_element_type=jnp.float32)
            for lane in range(0, BLOCK, 128):
                lanes = pl.ds(pl.multiple_of(start + lane, 128), 128)
                here = slice(lane, lane + 128)
                model_r = jnp.zeros((8, 128), jnp.float32)
                model_i = jnp.zeros((8, 128), jnp.float32)
                held = []
                for t in range(tiles):
                    sr, si = sky[0, pol, t, :, lanes], sky[1, pol, t, :, lanes]
                    mine = slice(t * 8, (t + 1) * 8)
                    other = slice(tall + t * 8, tall + (t + 1) * 8)
                    rr, ri = right[u, mine, here], right[u, other, here]
                    lr, li = left[u, mine, here], left[u, other, here]
                    zr = sr * rr + si * ri
                    zi = sr * ri - si * rr
                    model_r = model_r + (lr * zr + li * zi)
                    model_i = model_i + (li * zr - lr * zi)
                    held.append((zr, zi))
                all_r, all_i = model_r, model_i
                for lead in range(1, group):
                    all_r = all_r + pltpu.roll(model_r, lead * channels, 0)
                    all_i = all_i + pltpu.roll(model_i, lead * channels, 0)
                dr = vis[0, pol, :, lanes] - all_r
                di = vis[1, pol, :, lanes] - all_i
                for t in range(0, tiles, 2):
                    pair = held[t : t + 2]
                    values = (
                        [dr * zr - di * zi for zr, zi in pair],
                        [dr * zi + di * zr for zr, zi in pair],
                        [zr * zr + zi * zi for zr, zi in pair],
                    )
                    for i, value in enumerate(values):
                        high, low = split(jnp.concatenate(value, 0))
                        at = slice(i * tall + t * 8, i * tall + (t + 2) * 8)
                        parts[u, 0, at, here] = high
                        parts[u, 1, at, here] = low
            weight = gather_p[pl.ds(start, BLOCK), :]
            return jnp.dot(parts[u, 0], weight, preferred_element_type=jnp.float32) + jnp.dot(
                parts[u, 1], weight, preferred_element_type=jnp.float32
            )

        def several(b, carry):
            added = None
            for u in range(UNROLL):
                start = pl.multiple_of((b * UNROLL + u) * BLOCK, BLOCK)
                term = one_block(start, u)
                added = term if added is None else added + term
            total[...] += added
            return carry

        lax.fori_loop(0, blocks // UNROLL, several, 0)

        lane = lax.broadcasted_iota(jnp.int32, (tall, 128), 1)
        upper = jnp.where(lane < HALF, total[0:tall], total[tall : 2 * tall]).reshape(tiles, 8, 128)
        lower = total[2 * tall :].reshape(tiles, 8, 128)
        fresh = (upper + gain[pol] * lower + penalty * (cons[pol] - dual[pol])) / (lower + penalty)
        gain[pol] = fresh
        return fresh

    row = lax.broadcasted_iota(jnp.int32, (8, 128), 0) % channels

    def mixed(block, distance):
        out = None
        for shift in range(1 - channels, channels):
            offset = distance + shift + 4
            if offset < 0 or offset > 8:
                continue
            inside = (row + shift >= 0) & (row + shift < channels)
            weight = jnp.where(inside, kernel_taps[offset], 0.0)
            moved = block if shift == 0 else pltpu.roll(block, (-shift) % 8, 1)
            term = weight[None] * moved
            out = term if out is None else out + term
        return out

    def up_copy(it, pol):
        return pltpu.make_async_remote_copy(
            src_ref=summed.at[it, pol], dst_ref=from_low.at[it, pol],
            send_sem=send_sem.at[it, pol, 0], recv_sem=low_sem.at[it, pol],
            device_id={"chan": lax.rem(me + 1, count)}, device_id_type=MESH,
        )

    def down_copy(it, pol):
        return pltpu.make_async_remote_copy(
            src_ref=summed.at[it, pol], dst_ref=from_high.at[it, pol],
            send_sem=send_sem.at[it, pol, 1], recv_sem=high_sem.at[it, pol],
            device_id={"chan": lax.rem(me + count - 1, count)}, device_id_type=MESH,
        )

    def send(it, pol, fresh):
        summed[it, pol] = fresh + dual[pol]

        @pl.when(me < count - 1)
        def _():
            up_copy(it, pol).start()

        @pl.when(me > 0)
        def _():
            down_copy(it, pol).start()

    def smooth(it, pol):
        own = mixed(summed[it, pol], 0)

        @pl.when(me > 0)
        def _():
            up_copy(it, pol).wait_recv()

        @pl.when(me < count - 1)
        def _():
            down_copy(it, pol).wait_recv()

        fresh = own + mixed(from_low[it, pol], -channels) + mixed(from_high[it, pol], channels)
        gap = gain[pol] - fresh
        moved = fresh - cons[pol]
        dual[pol] = dual[pol] + gap
        cons[pol] = fresh
        sums[2 * it : 2 * it + 1] += jnp.sum(jnp.sum(gap * gap, 0), 0, keepdims=True)
        sums[2 * it + 1 : 2 * it + 2] += jnp.sum(jnp.sum(moved * moved, 0), 0, keepdims=True)

    def norm_copy(step):
        return pltpu.make_async_remote_copy(
            src_ref=sums, dst_ref=slots.at[me],
            send_sem=norm_send.at[step], recv_sem=norm_recv.at[step],
            device_id={"chan": lax.rem(me + step, count)}, device_id_type=MESH,
        )

    def put(target, state, pol):
        for part in range(2):
            lanes = slice(part * HALF, part * HALF + width)
            for lead in range(group):
                rows = slice(lead * channels, (lead + 1) * channels)
                for tile in range(tiles):
                    target[part, pol, tile * group + lead] = state[pol, tile, rows, lanes]

    for it in range(ITERS):
        for pol in range(pols):
            if it == 0:
                unpack(pol)
            else:
                smooth(it - 1, pol)
            fresh = solve(pol)
            if it == 0 and pol == 0:
                pl.semaphore_wait(barrier, count - 1)
            send(it, pol, fresh)
    for pol in range(pols):
        put(jones_out, gain, pol)
    for pol in range(pols):
        smooth(ITERS - 1, pol)

    slots[pl.ds(me, 1)] = sums[...][None]
    for step in range(1, count):
        norm_copy(step).start()
    for pol in range(pols):
        put(consensus_out, cons, pol)
        put(duals_out, dual, pol)

    for it in range(ITERS):
        for pol in range(pols):

            @pl.when(me < count - 1)
            def _():
                up_copy(it, pol).wait_send()

            @pl.when(me > 0)
            def _():
                down_copy(it, pol).wait_send()

    for step in range(1, count):
        norm_copy(step).wait()
    gathered = slots[0]
    for j in range(1, count):
        gathered = gathered + slots[j]
    folded = jnp.sum(gathered, axis=1, keepdims=True) * (1.0 / entries)
    for it in range(ITERS):
        norms_out[it : it + 1, 0:1] = folded[2 * it : 2 * it + 1]
        norms_out[it : it + 1, 1:2] = folded[2 * it + 1 : 2 * it + 2] * (penalty * penalty)


def solution(mesh):
    count = mesh.shape["chan"]

    def local(visibility, coherency, jones_start, duals_start):
        _, pols, dirs, channels, width = jones_start.shape
        pairs = visibility.shape[-1]
        times = visibility.shape[3]
        assert times == 1 and channels == 4 and dirs % 4 == 0 and width <= HALF - 2
        blocks = pl.cdiv(pairs, BLOCK * UNROLL) * UNROLL
        long = blocks * BLOCK
        tiles = dirs * channels // 8
        tall = tiles * 8
        entries = jones_start.size * count
        sky = coherency.transpose(0, 1, 2, 4, 3, 5).reshape(2, pols, dirs, channels, pairs)
        state = jax.ShapeDtypeStruct(jones_start.shape, jnp.float32)
        f32, bf16 = jnp.float32, jnp.bfloat16
        packed = (pols, tiles, 8, 2 * HALF)
        return pl.pallas_call(
            functools.partial(kernel, count, (pols, dirs, channels, width, pairs, blocks, entries)),
            out_shape=(state, state, state, jax.ShapeDtypeStruct((ITERS, 2), f32)),
            in_specs=[pl.BlockSpec(memory_space=pl.ANY)] * 4,
            out_specs=tuple([pl.BlockSpec(memory_space=pltpu.VMEM)] * 4),
            scratch_shapes=[
                pltpu.VMEM(visibility.shape, f32),
                pltpu.VMEM(sky.shape, bf16),
                pltpu.VMEM(jones_start.shape, f32),
                pltpu.VMEM(duals_start.shape, f32),
                pltpu.VMEM((2, pols, 8, long), f32),
                pltpu.VMEM((2, pols, tiles, 8, long), f32),
                pltpu.VMEM((HALF, long), bf16),
                pltpu.VMEM((HALF, long), bf16),
                pltpu.VMEM((long, 2 * HALF), bf16),
                pltpu.VMEM((pols, 2 * tall, 4 * HALF), bf16),
                pltpu.VMEM((UNROLL, 2 * tall, BLOCK), f32),
                pltpu.VMEM((UNROLL, 2 * tall, BLOCK), f32),
                pltpu.VMEM((UNROLL, 2, 3 * tall, BLOCK), bf16),
                pltpu.VMEM(packed, f32),
                pltpu.VMEM(packed, f32),
                pltpu.VMEM(packed, f32),
                pltpu.VMEM((3 * tall, 2 * HALF), f32),
                pltpu.VMEM((ITERS,) + packed, f32),
                pltpu.VMEM((ITERS,) + packed, f32),
                pltpu.VMEM((ITERS,) + packed, f32),
                pltpu.VMEM((8, 2 * HALF), f32),
                pltpu.VMEM((count, 8, 2 * HALF), f32),
                pltpu.SemaphoreType.DMA((3,)),
                pltpu.SemaphoreType.DMA((2, pols)),
                pltpu.SemaphoreType.DMA((ITERS, pols, 2)),
                pltpu.SemaphoreType.DMA((ITERS, pols)),
                pltpu.SemaphoreType.DMA((ITERS, pols)),
                pltpu.SemaphoreType.DMA((count,)),
                pltpu.SemaphoreType.DMA((count,)),
            ],
            compiler_params=pltpu.CompilerParams(
                collective_id=0, has_side_effects=True, vmem_limit_bytes=60 * 1024 * 1024
            ),
        )(visibility, sky, jones_start, duals_start)

    placed = (
        P(None, None, "chan", "slot", None),
        P(None, None, None, "chan", "slot", None),
        P(None, None, "slot", "chan", None),
        P(None, None, "slot", "chan", None),
    )
    return jax.shard_map(
        local,
        mesh=mesh,
        in_specs=placed,
        out_specs=(
            P(None, None, "slot", "chan", None),
            P(None, None, "slot", "chan", None),
            P(None, None, "slot", "chan", None),
            P("slot", None),
        ),
        check_vma=False,
    )
```

```python
import functools

import jax
import jax.numpy as jnp
from jax import lax
from jax.experimental import pallas as pl
from jax.experimental.pallas import tpu as pltpu
from jax.sharding import PartitionSpec as P

ITERS = 2
HALF = 64
BLOCK = 256
MESH = pl.DeviceIdType.MESH

penalty = 8.0
kernel_taps = (0.04, 0.06, 0.1, 0.15, 0.3, 0.15, 0.1, 0.06, 0.04)


def split(value):
    high = value.astype(jnp.bfloat16)
    return high, (value - high.astype(jnp.float32)).astype(jnp.bfloat16)


def spread_tables(width, blocks, spread_p, spread_q, gather_p):
    def fill(b, carry):
        start = pl.multiple_of(b * BLOCK, BLOCK)
        pair = (lax.broadcasted_iota(jnp.int32, (HALF, BLOCK), 1) + start).astype(jnp.float32)
        station = lax.broadcasted_iota(jnp.int32, (HALF, BLOCK), 0).astype(jnp.float32)
        first = jnp.floor((pair + 0.5) * (1.0 / width))
        second = pair - first * width
        keep = (first != second) & (first < width)
        for table, which in ((spread_p, first), (spread_q, second)):
            chosen = jnp.where((which == station) & keep, 1.0, 0.0).astype(jnp.bfloat16)
            table[0:HALF, pl.ds(start, BLOCK)] = chosen
            table[HALF:, pl.ds(start, BLOCK)] = chosen
        pair = (lax.broadcasted_iota(jnp.int32, (BLOCK, 2 * HALF), 0) + start).astype(jnp.float32)
        station = (lax.broadcasted_iota(jnp.int32, (BLOCK, 2 * HALF), 1) & (HALF - 1)).astype(jnp.float32)
        inside = pair - station * width
        keep = (inside >= 0.0) & (inside < width) & (inside != station) & (station < width)
        gather_p[pl.ds(start, BLOCK), :] = jnp.where(keep, 1.0, 0.0).astype(jnp.bfloat16)
        return carry

    lax.fori_loop(0, blocks, fill, 0)


def kernel(
    count, dims,
    vis_in, sky_in, jones_in, duals_in,
    jones_out, consensus_out, duals_out, norms_out,
    vis_raw, sky_raw, jones_raw, duals_raw,
    vis, sky, spread_p, spread_q, gather_p, lhs, left, right, parts,
    gain, cons, dual, summed, from_low, from_high, sums, slots,
    load_sem, sky_sem, send_sem, low_sem, high_sem, norm_send, norm_recv,
):
    pols, dirs, channels, width, pairs, blocks, entries = dims
    me = lax.axis_index("chan")
    group = 8 // channels
    tiles = dirs // group
    tall = tiles * 8

    loads = [
        pltpu.make_async_copy(source, target, load_sem.at[i])
        for i, (source, target) in enumerate(((vis_in, vis_raw), (jones_in, jones_raw), (duals_in, duals_raw)))
    ]
    sky_loads = [
        [pltpu.make_async_copy(sky_in.at[part, pol], sky_raw.at[part, pol], sky_sem.at[part, pol]) for part in range(2)]
        for pol in range(pols)
    ]
    for copy in loads + [copy for per_pol in sky_loads for copy in per_pol]:
        copy.start()

    from_low[...] = jnp.zeros_like(from_low)
    from_high[...] = jnp.zeros_like(from_high)
    barrier = pltpu.get_barrier_semaphore()
    for step in range(1, count):
        pl.semaphore_signal(barrier, inc=1, device_id={"chan": lax.rem(me + step, count)}, device_id_type=MESH)

    spread_tables(width, blocks, spread_p, spread_q, gather_p)
    tail = pairs // 128 * 128
    edge = blocks * BLOCK - tail
    vis[:, :, :, pl.ds(tail, edge)] = jnp.zeros((2, pols, 8, edge), jnp.float32)
    sky[:, :, :, :, pl.ds(tail, edge)] = jnp.zeros((2, pols, tiles, 8, edge), jnp.float32)
    gain[...] = jnp.zeros_like(gain)
    dual[...] = jnp.zeros_like(dual)
    sums[...] = jnp.zeros_like(sums)
    for copy in loads:
        copy.wait()
    for part in range(2):
        for pol in range(pols):
            for row in range(8):
                vis[part, pol, row : row + 1, 0:pairs] = vis_raw[part, pol, row % channels]
            for lead in range(group):
                rows = slice(lead * channels, (lead + 1) * channels)
                lanes = slice(part * HALF, part * HALF + width)
                for tile in range(tiles):
                    gain[pol, tile, rows, lanes] = jones_raw[part, pol, tile * group + lead]
                    dual[pol, tile, rows, lanes] = duals_raw[part, pol, tile * group + lead]
    cons[...] = gain[...]

    def unpack(pol):
        for copy in sky_loads[pol]:
            copy.wait()

        def one(tile, carry):
            for part in range(2):
                for lead in range(group):
                    rows = slice(lead * channels, (lead + 1) * channels)
                    sky[part, pol, tile, rows, 0:pairs] = sky_raw[part, pol, tile * group + lead].astype(jnp.float32)
            return carry

        lax.fori_loop(0, tiles, one, 0)

    def solve(pol):
        now = gain[pol].reshape(tall, 128)
        lane = lax.broadcasted_iota(jnp.int32, (tall, 128), 1)
        high = now.astype(jnp.bfloat16).astype(jnp.float32)
        low = now - high
        lhs[pol, 0:tall] = jnp.where(lane < HALF, high, pltpu.roll(low, HALF, 1)).astype(jnp.bfloat16)
        lhs[pol, tall:] = jnp.where(lane < HALF, pltpu.roll(high, HALF, 1), low).astype(jnp.bfloat16)
        right[...] = jnp.dot(lhs[pol], spread_q[...], preferred_element_type=jnp.float32)
        left[...] = jnp.dot(lhs[pol], spread_p[...], preferred_element_type=jnp.float32)

        def one_block(b, carry):
            for sub in range(0, BLOCK, 128):
                lanes = pl.ds(pl.multiple_of(b * BLOCK + sub, 128), 128)
                model_r = jnp.zeros((8, 128), jnp.float32)
                model_i = jnp.zeros((8, 128), jnp.float32)
                held = []
                for t in range(tiles):
                    sr, si = sky[0, pol, t, :, lanes], sky[1, pol, t, :, lanes]
                    mine = slice(t * 8, (t + 1) * 8)
                    other = slice(tall + t * 8, tall + (t + 1) * 8)
                    rr, ri = right[mine, lanes], right[other, lanes]
                    lr, li = left[mine, lanes], left[other, lanes]
                    zr = sr * rr + si * ri
                    zi = sr * ri - si * rr
                    model_r = model_r + (lr * zr + li * zi)
                    model_i = model_i + (li * zr - lr * zi)
                    held.append((zr, zi))
                all_r, all_i = model_r, model_i
                for lead in range(1, group):
                    all_r = all_r + pltpu.roll(model_r, lead * channels, 0)
                    all_i = all_i + pltpu.roll(model_i, lead * channels, 0)
                dr = vis[0, pol, :, lanes] - all_r
                di = vis[1, pol, :, lanes] - all_i
                for t in range(0, tiles, 2):
                    pair = held[t : t + 2]
                    values = (
                        [dr * zr - di * zi for zr, zi in pair],
                        [dr * zi + di * zr for zr, zi in pair],
                        [zr * zr + zi * zi for zr, zi in pair],
                    )
                    for i, value in enumerate(values):
                        upper, rest = split(jnp.concatenate(value, 0))
                        parts[i * tall + t * 8 : i * tall + (t + 2) * 8, lanes] = upper
                        parts[(3 + i) * tall + t * 8 : (3 + i) * tall + (t + 2) * 8, lanes] = rest
            return carry

        lax.fori_loop(0, blocks, one_block, 0)

        both = jnp.dot(parts[...], gather_p[...], preferred_element_type=jnp.float32)
        total = both[0 : 3 * tall] + both[3 * tall :]
        upper = jnp.where(lane < HALF, total[0:tall], total[tall : 2 * tall]).reshape(tiles, 8, 128)
        lower = total[2 * tall :].reshape(tiles, 8, 128)
        fresh = (upper + gain[pol] * lower + penalty * (cons[pol] - dual[pol])) / (lower + penalty)
        gain[pol] = fresh
        return fresh

    row = lax.broadcasted_iota(jnp.int32, (8, 128), 0) % channels

    def mixed(block, distance):
        out = None
        for shift in range(1 - channels, channels):
            offset = distance + shift + 4
            if offset < 0 or offset > 8:
                continue
            inside = (row + shift >= 0) & (row + shift < channels)
            weight = jnp.where(inside, kernel_taps[offset], 0.0)
            moved = block if shift == 0 else pltpu.roll(block, (-shift) % 8, 1)
            term = weight[None] * moved
            out = term if out is None else out + term
        return out

    def up_copy(it, pol):
        return pltpu.make_async_remote_copy(
            src_ref=summed.at[it, pol], dst_ref=from_low.at[it, pol],
            send_sem=send_sem.at[it, pol, 0], recv_sem=low_sem.at[it, pol],
            device_id={"chan": lax.rem(me + 1, count)}, device_id_type=MESH,
        )

    def down_copy(it, pol):
        return pltpu.make_async_remote_copy(
            src_ref=summed.at[it, pol], dst_ref=from_high.at[it, pol],
            send_sem=send_sem.at[it, pol, 1], recv_sem=high_sem.at[it, pol],
            device_id={"chan": lax.rem(me + count - 1, count)}, device_id_type=MESH,
        )

    def send(it, pol, fresh):
        summed[it, pol] = fresh + dual[pol]

        @pl.when(me < count - 1)
        def _():
            up_copy(it, pol).start()

        @pl.when(me > 0)
        def _():
            down_copy(it, pol).start()

    def smooth(it, pol):
        own = mixed(summed[it, pol], 0)

        @pl.when(me > 0)
        def _():
            up_copy(it, pol).wait_recv()

        @pl.when(me < count - 1)
        def _():
            down_copy(it, pol).wait_recv()

        fresh = own + mixed(from_low[it, pol], -channels) + mixed(from_high[it, pol], channels)
        gap = gain[pol] - fresh
        moved = fresh - cons[pol]
        dual[pol] = dual[pol] + gap
        cons[pol] = fresh
        sums[2 * it : 2 * it + 1] += jnp.sum(jnp.sum(gap * gap, 0), 0, keepdims=True)
        sums[2 * it + 1 : 2 * it + 2] += jnp.sum(jnp.sum(moved * moved, 0), 0, keepdims=True)

    def norm_copy(step):
        return pltpu.make_async_remote_copy(
            src_ref=sums, dst_ref=slots.at[me],
            send_sem=norm_send.at[step], recv_sem=norm_recv.at[step],
            device_id={"chan": lax.rem(me + step, count)}, device_id_type=MESH,
        )

    def put(target, state, pol):
        for part in range(2):
            lanes = slice(part * HALF, part * HALF + width)
            for lead in range(group):
                rows = slice(lead * channels, (lead + 1) * channels)
                for tile in range(tiles):
                    target[part, pol, tile * group + lead] = state[pol, tile, rows, lanes]

    for it in range(ITERS):
        for pol in range(pols):
            if it == 0:
                unpack(pol)
            else:
                smooth(it - 1, pol)
            fresh = solve(pol)
            if it == 0 and pol == 0:
                pl.semaphore_wait(barrier, count - 1)
            send(it, pol, fresh)
    for pol in range(pols):
        put(jones_out, gain, pol)
    for pol in range(pols):
        smooth(ITERS - 1, pol)

    slots[pl.ds(me, 1)] = sums[...][None]
    for step in range(1, count):
        norm_copy(step).start()
    for pol in range(pols):
        put(consensus_out, cons, pol)
        put(duals_out, dual, pol)

    for it in range(ITERS):
        for pol in range(pols):

            @pl.when(me < count - 1)
            def _():
                up_copy(it, pol).wait_send()

            @pl.when(me > 0)
            def _():
                down_copy(it, pol).wait_send()

    for step in range(1, count):
        norm_copy(step).wait()
    gathered = slots[0]
    for j in range(1, count):
        gathered = gathered + slots[j]
    folded = jnp.sum(gathered, axis=1, keepdims=True) * (1.0 / entries)
    for it in range(ITERS):
        norms_out[it : it + 1, 0:1] = folded[2 * it : 2 * it + 1]
        norms_out[it : it + 1, 1:2] = folded[2 * it + 1 : 2 * it + 2] * (penalty * penalty)


def solution(mesh):
    count = mesh.shape["chan"]

    def local(visibility, coherency, jones_start, duals_start):
        _, pols, dirs, channels, width = jones_start.shape
        pairs = visibility.shape[-1]
        times = visibility.shape[3]
        assert times == 1 and channels == 4 and dirs % 4 == 0 and width <= HALF - 2
        blocks = pl.cdiv(pairs, BLOCK)
        long = blocks * BLOCK
        tiles = dirs * channels // 8
        tall = tiles * 8
        entries = jones_start.size * count
        sky = coherency.transpose(0, 1, 2, 4, 3, 5).reshape(2, pols, dirs, channels, pairs)
        state = jax.ShapeDtypeStruct(jones_start.shape, jnp.float32)
        f32, bf16 = jnp.float32, jnp.bfloat16
        packed = (pols, tiles, 8, 2 * HALF)
        return pl.pallas_call(
            functools.partial(kernel, count, (pols, dirs, channels, width, pairs, blocks, entries)),
            out_shape=(state, state, state, jax.ShapeDtypeStruct((ITERS, 2), f32)),
            in_specs=[pl.BlockSpec(memory_space=pl.ANY)] * 4,
            out_specs=tuple([pl.BlockSpec(memory_space=pltpu.VMEM)] * 4),
            scratch_shapes=[
                pltpu.VMEM(visibility.shape, f32),
                pltpu.VMEM(sky.shape, bf16),
                pltpu.VMEM(jones_start.shape, f32),
                pltpu.VMEM(duals_start.shape, f32),
                pltpu.VMEM((2, pols, 8, long), f32),
                pltpu.VMEM((2, pols, tiles, 8, long), f32),
                pltpu.VMEM((2 * HALF, long), bf16),
                pltpu.VMEM((2 * HALF, long), bf16),
                pltpu.VMEM((long, 2 * HALF), bf16),
                pltpu.VMEM((pols, 2 * tall, 2 * HALF), bf16),
                pltpu.VMEM((2 * tall, long), f32),
                pltpu.VMEM((2 * tall, long), f32),
                pltpu.VMEM((6 * tall, long), bf16),
                pltpu.VMEM(packed, f32),
                pltpu.VMEM(packed, f32),
                pltpu.VMEM(packed, f32),
                pltpu.VMEM((ITERS,) + packed, f32),
                pltpu.VMEM((ITERS,) + packed, f32),
                pltpu.VMEM((ITERS,) + packed, f32),
                pltpu.VMEM((8, 2 * HALF), f32),
                pltpu.VMEM((count, 8, 2 * HALF), f32),
                pltpu.SemaphoreType.DMA((3,)),
                pltpu.SemaphoreType.DMA((2, pols)),
                pltpu.SemaphoreType.DMA((ITERS, pols, 2)),
                pltpu.SemaphoreType.DMA((ITERS, pols)),
                pltpu.SemaphoreType.DMA((ITERS, pols)),
                pltpu.SemaphoreType.DMA((count,)),
                pltpu.SemaphoreType.DMA((count,)),
            ],
            compiler_params=pltpu.CompilerParams(
                collective_id=0, has_side_effects=True, vmem_limit_bytes=60 * 1024 * 1024
            ),
        )(visibility, sky, jones_start, duals_start)

    placed = (
        P(None, None, "chan", "slot", None),
        P(None, None, None, "chan", "slot", None),
        P(None, None, "slot", "chan", None),
        P(None, None, "slot", "chan", None),
    )
    return jax.shard_map(
        local,
        mesh=mesh,
        in_specs=placed,
        out_specs=(
            P(None, None, "slot", "chan", None),
            P(None, None, "slot", "chan", None),
            P(None, None, "slot", "chan", None),
            P("slot", None),
        ),
        check_vma=False,
    )
```
